1024 devices in a mesh: fsdp: 64 (over z, x), row: 16 (over y, core).
Axes of the slice: x: 4, y: 8, z: 16, core: 2. Of those that a mesh axis runs over, the one named last changes fastest.
Arguments:
- weight: bfloat16 [8192, 26624], P('row', 'fsdp'), may hold values from -0.3125 to 0.3125
- momentum: bfloat16 [8192, 26624], P('row', 'fsdp'), may hold values from -6 to 6
- gradient: bfloat16 [8192, 26624], P('row', 'fsdp'), may hold values from -6 to 6
- basis: bfloat16 [26624, 256], P('fsdp'), may hold values from -0.0390625 to 0.0390625
Outputs:
- weight_new: bfloat16 [8192, 26624], P('row', 'fsdp')
- momentum_new: bfloat16 [8192, 26624], P('row', 'fsdp')
- basis_new: bfloat16 [26624, 256], P('fsdp')
The draws below stay inside these ranges and needn't reach their ends.
All inputs are finite; a program needn't handle non-finite values.
Results may differ from the reference program's by a relative error of at most 0.009.
Values may be sent and summed in bfloat16 or wider, within the bound.
A program may use at most 32 MiB of HBM per device.

```python
import jax
import jax.numpy as jnp
from jax import lax

D = 8192
FF = 26624
RANK = 256


def block_scale(key, dims, split, smallest, largest):
    factor_of, own = 1.0, jax.random.fold_in(key, 6)
    for position, shards_of in split:
        draws = jnp.exp(jax.random.uniform(jax.random.fold_in(own, position), (shards_of,), jnp.float32, smallest / len(split), largest / len(split)))
        factor_of = factor_of * jnp.repeat(draws, dims[position] // shards_of).reshape([-1 if axis == position else 1 for axis in range(len(dims))])
    return factor_of


def centred(rng, shape, scale, most, shards=(), kind=jnp.bfloat16):
    entries = jax.random.normal(rng, shape, jnp.float32) * scale
    if len(shards) > 0:
        entries = block_scale(rng, shape, shards, -0.22, 0.18) * entries
    return jnp.clip(entries, min=-most, max=most).astype(kind)


def setup_inputs(seed: int = 0) -> dict:
    key_list = jax.random.split(jax.random.key(seed), 5)
    return {
        "weight": centred(key_list[0], (D, FF), 0.02, 0.3125, ((0, 16), (1, 64))),
        "momentum": centred(key_list[1], (D, FF), 1.0, 6.0, ((0, 16), (1, 64))),
        "gradient": centred(key_list[2], (D, FF), 1.0, 6.0, ((0, 16), (1, 64))),
        "basis": centred(key_list[3], (FF, RANK), FF ** -0.5, 0.0390625, ((0, 64),)),
    }


def reference(weight, momentum, gradient, basis):
    buffer = (momentum.astype(jnp.float32) + gradient.astype(jnp.float32)).astype(jnp.bfloat16)
    power = jnp.dot(buffer.astype(jnp.float32), basis.astype(jnp.float32), preferred_element_type=jnp.float32)
    gram = jnp.dot(power.T.astype(jnp.float32), power.astype(jnp.float32), precision=lax.Precision.HIGHEST, preferred_element_type=jnp.float32)
    lower = jnp.linalg.cholesky(gram)
    ortho = lax.linalg.triangular_solve(lower, power, left_side=False, lower=True, transpose_a=True).astype(jnp.bfloat16)
    right = jnp.dot(buffer.T.astype(jnp.float32), ortho.astype(jnp.float32), preferred_element_type=jnp.float32)
    colsq = lax.optimization_barrier(jnp.sum(right * right, axis=0))
    right_b = right.astype(jnp.bfloat16)
    basis_new = (right_b.astype(jnp.float32) / jnp.sqrt(colsq + 1e-06)).astype(jnp.bfloat16)
    feedback = jnp.dot(ortho.astype(jnp.float32), right_b.T.astype(jnp.float32), preferred_element_type=jnp.float32)
    momentum_new = (buffer.astype(jnp.float32) - 0.5 * feedback).astype(jnp.bfloat16)
    coeff = 0.3 * (D * FF / RANK) ** 0.5 / 50.0
    update = jnp.dot(ortho.astype(jnp.float32), basis_new.T.astype(jnp.float32), preferred_element_type=jnp.float32)
    weight_new = (weight.astype(jnp.float32) - coeff * update).astype(jnp.bfloat16)
    return (weight_new, momentum_new, basis_new)
```

```python
import functools

import jax
import jax.numpy as jnp
from jax import lax
from jax.experimental import pallas as pl
from jax.experimental.pallas import tpu as pltpu
from jax.sharding import Mesh
from jax.sharding import PartitionSpec as P

D = 8192
FF = 26624
RANK = 256
Z, X, Y, C = "fsdp_0", "fsdp_1", "row_0", "row_1"
FSDP = (Z, X)
ROW = (Y, C)
SIZES = (16, 4, 8, 2)
BF, F32 = jnp.bfloat16, jnp.float32
PAD = 512
MESH = pl.DeviceIdType.MESH


def far_first(n):
    return sorted(range(1, n), key=lambda d: -min(d, n - d))


def far_pairs(n, m):
    pairs = [(a, b) for a in range(n) for b in range(m) if a or b]
    return sorted(pairs, key=lambda p: -(min(p[0], n - p[0]) + min(p[1], m - p[1])))


def rows(start, size):
    return pl.ds(pl.multiple_of(start, size), size)


def wrap(i, n):
    return lax.rem(i, n)


def remote(src, dst, send, recv, peer):
    return pltpu.make_async_remote_copy(
        src_ref=src, dst_ref=dst, send_sem=send, recv_sem=recv, device_id=peer, device_id_type=MESH
    )


def power_kernel(
    sizes, m_ref, g_ref, b_ref, buft_ref, p_ref, gram_ref,
    wide, part, xbuf, zpart, zbuf, pbuf, gp, gbuf, gh, ybuf, gall,
    xs, xr, zs, zr, zs2, zr2, xs2, xr2, cs, cr, ys, yr, ys2, yr2, cs2, cr2,
):
    nz, nx, ny, nc = sizes
    z, x, y, c = (lax.axis_index(a) for a in (Z, X, Y, C))
    barrier = pltpu.get_barrier_semaphore()
    for axis, me, n in ((Z, z, nz), (X, x, nx), (Y, y, ny), (C, c, nc)):
        for d in far_first(n):
            pl.semaphore_signal(barrier, inc=1, device_id={axis: wrap(me + d, n)}, device_id_type=MESH)

    buffer = (m_ref[...].astype(F32) + g_ref[...].astype(F32)).astype(BF)
    part[...] = jnp.dot(buffer, b_ref[...], preferred_element_type=F32).astype(BF)
    pl.semaphore_wait(barrier, nz + nx + ny + nc - 4)

    nloc = part.shape[0]
    q = nloc // nx
    copies = []
    for d in far_first(nx):
        peer = wrap(x + d, nx)
        cp = remote(part.at[rows(peer * q, q)], xbuf.at[d], xs.at[d], xr.at[d], {X: peer})
        cp.start()
        copies.append(cp)
    wide[...] = jnp.zeros_like(wide)
    wide[:, : buffer.shape[1]] = buffer
    for cp in copies:
        cp.wait()
    total = part[rows(x * q, q), :].astype(F32)
    for d in range(1, nx):
        total += xbuf[d].astype(F32)
    zpart[...] = total.astype(BF)

    th = 2 * q // nz

    def tile(i):
        return (rows(lax.div(i, 2) * th, th), rows(lax.rem(i, 2) * 128, 128))

    copies = []
    for d in far_first(nz):
        peer = wrap(z + d, nz)
        cp = remote(zpart.at[tile(peer)], zbuf.at[d], zs.at[d], zr.at[d], {Z: peer})
        cp.start()
        copies.append(cp)
    buft_ref[...] = wide[...].T
    for cp in copies:
        cp.wait()
    own = zpart[tile(z)].astype(F32)
    for d in range(1, nz):
        own += zbuf[d].astype(F32)

    def ptile(i):
        return (rows(x * q + lax.div(i, 2) * th, th), rows(lax.rem(i, 2) * 128, 128))

    pbuf[ptile(z)] = own.astype(BF)
    copies = []
    for d in far_first(nz):
        cp = remote(pbuf.at[ptile(z)], pbuf.at[ptile(z)], zs2.at[d], zr2.at[d], {Z: wrap(z + d, nz)})
        cp.start()
        copies.append(cp)
    for d, cp in zip(far_first(nz), copies):
        cp.wait_send()
        src = wrap(z - d + nz, nz)
        remote(pbuf.at[ptile(src)], pbuf.at[ptile(src)], zs2.at[d], zr2.at[d], {Z: src}).wait_recv()

    mine = rows(x * q, q)
    copies = []
    for d in far_first(nx):
        cp = remote(pbuf.at[mine], pbuf.at[mine], xs2.at[d], xr2.at[d], {X: wrap(x + d, nx)})
        cp.start()
        copies.append(cp)
    gp[...] = gram_of(pbuf[mine, :])
    for d in sorted(range(1, nx), key=lambda d: min(d, nx - d)):
        src = wrap(x - d + nx, nx)
        there = rows(src * q, q)
        remote(pbuf.at[there], pbuf.at[there], xs2.at[d], xr2.at[d], {X: src}).wait_recv()
        gp[...] += gram_of(pbuf[there, :])
    for cp in copies:
        cp.wait_send()

    h = RANK // 2
    peer = {C: 1 - c}
    cp = remote(gp.at[rows((1 - c) * h, h)], gbuf, cs, cr, peer)
    cp.start()
    p_ref[...] = pbuf[...]
    cp.wait()
    gh[...] = gp[rows(c * h, h), :] + gbuf[...]

    s = h // ny
    copies = []
    for d in far_first(ny):
        to = wrap(y + d, ny)
        cp = remote(gh.at[rows(to * s, s)], ybuf.at[d], ys.at[d], yr.at[d], {Y: to})
        cp.start()
        copies.append(cp)
    for cp in copies:
        cp.wait()
    own = gh[rows(y * s, s), :]
    for d in range(1, ny):
        own += ybuf[d]

    def slot(i):
        return rows(c * h + i * s, s)

    gall[slot(y), :] = own
    copies = []
    for d in far_first(ny):
        cp = remote(gall.at[slot(y)], gall.at[slot(y)], ys2.at[d], yr2.at[d], {Y: wrap(y + d, ny)})
        cp.start()
        copies.append(cp)
    for d, cp in zip(far_first(ny), copies):
        cp.wait_send()
        src = wrap(y - d + ny, ny)
        remote(gall.at[slot(src)], gall.at[slot(src)], ys2.at[d], yr2.at[d], {Y: src}).wait_recv()
    half = rows(c * h, h)
    cp = remote(gall.at[half], gall.at[half], cs2, cr2, peer)
    cp.start()
    cp.wait_send()
    other = rows((1 - c) * h, h)
    remote(gall.at[other], gall.at[other], cs2, cr2, peer).wait_recv()
    gram_ref[...] = gall[...]


def gram_of(block):
    return lax.dot_general(block, block, (((0,), (0,)), ((), ())), preferred_element_type=F32)


def full(a, b, dims):
    return lax.dot_general(
        a, b, (dims, ((), ())), precision=lax.Precision.HIGHEST, preferred_element_type=F32
    )


def factor_kernel(g_ref, hi_ref, lo_ref, sym, low):
    n = RANK
    i = lax.broadcasted_iota(jnp.int32, (n, n), 0)
    j = lax.broadcasted_iota(jnp.int32, (n, n), 1)
    gram = g_ref[...]
    diag = jnp.where(i == j, gram, 0.0)
    across = lax.rsqrt(jnp.sum(diag, axis=0, keepdims=True))
    down = lax.rsqrt(jnp.sum(diag, axis=1, keepdims=True))
    sym[...] = gram * across * down
    eye = jnp.where(i == j, 1.0, 0.0)

    def phi(e):
        return jnp.where(i > j, e, jnp.where(i == j, 0.5 * e, 0.0))

    low[...] = eye - phi(sym[...] - eye)
    small = 1e-4

    def more(state):
        step, err = state
        return jnp.logical_and(step < 12, err > small)

    def newton(state):
        step, _ = state
        inv = low[...]
        e = full(full(inv, sym[...], ((1,), (0,))), inv, ((1,), (1,)))
        e = e - jnp.where(i == j, 1.0, 0.0)
        low[...] = inv - full(phi(e), inv, ((1,), (0,)))
        return step + 1, jnp.sum(e * e)

    _, err = lax.while_loop(more, newton, (0, jnp.float32(1.0)))

    @pl.when(jnp.logical_not(err <= small))
    def _():
        sym[...] = g_ref[...] * across * down
        low[...] = jnp.where(i == j, 1.0, 0.0)
        lane = lax.broadcasted_iota(jnp.int32, (1, n), 1)
        line = lax.broadcasted_iota(jnp.int32, (n, 1), 0)

        def column(k, _):
            pivots = sym[pl.ds(k, 1), :]
            pivot = jnp.sum(jnp.where(lane == k, pivots, 0.0), axis=1, keepdims=True)
            inverse = low[pl.ds(k, 1), :]
            here = sym[...]
            col = jnp.sum(jnp.where(j == k, here, 0.0), axis=1, keepdims=True)
            times = jnp.where(line > k, col / pivot, 0.0)
            sym[...] = here - times * pivots
            low[...] = low[...] - times * inverse
            return 0

        lax.fori_loop(0, n, column, 0)
        pivot = jnp.sum(jnp.where(i == j, sym[...], 0.0), axis=1, keepdims=True)
        low[...] = low[...] * lax.rsqrt(pivot)

    inv = low[...] * across
    hi = inv.astype(BF)
    hi_ref[...] = hi
    lo_ref[...] = (inv - hi.astype(F32)).astype(BF)


def right_kernel(
    sizes, p_ref, hi_ref, lo_ref, buft_ref, ortho_ref, right_ref, colsq_ref,
    part, cbuf, half, ybuf, rall, sq1, sq2,
    cs, cr, ys, yr, ys2, yr2, cs2, cr2, s1, r1, s2, r2,
):
    nz, nx, ny, nc = sizes
    z, x, y, c = (lax.axis_index(a) for a in (Z, X, Y, C))
    barrier = pltpu.get_barrier_semaphore()
    plane = far_pairs(ny, nx)
    line = far_pairs(nz, nc)
    for dz, dc in line:
        to = {Z: wrap(z + dz, nz), C: wrap(c + dc, nc)}
        pl.semaphore_signal(barrier, inc=1, device_id=to, device_id_type=MESH)
    for dy, dx in plane:
        to = {Y: wrap(y + dy, ny), X: wrap(x + dx, nx)}
        pl.semaphore_signal(barrier, inc=1, device_id=to, device_id_type=MESH)

    across = (((1,), (1,)), ((), ()))
    power = p_ref[...]
    ortho = lax.dot_general(power, hi_ref[...], across, preferred_element_type=F32)
    ortho += lax.dot_general(power, lo_ref[...], across, preferred_element_type=F32)
    ortho = ortho.astype(BF)
    ortho_ref[...] = ortho
    part[...] = jnp.dot(buft_ref[...], ortho, preferred_element_type=F32).astype(BF)
    pl.semaphore_wait(barrier, len(plane) + len(line))

    h = PAD // 2
    peer = {C: 1 - c}
    cp = remote(part.at[rows((1 - c) * h, h)], cbuf, cs, cr, peer)
    cp.start()
    cp.wait()
    half[...] = (part[rows(c * h, h), :].astype(F32) + cbuf[...].astype(F32)).astype(BF)

    s = h // ny
    copies = []
    for d in far_first(ny):
        to = wrap(y + d, ny)
        cp = remote(half.at[rows(to * s, s)], ybuf.at[d], ys.at[d], yr.at[d], {Y: to})
        cp.start()
        copies.append(cp)
    for cp in copies:
        cp.wait()
    own = half[rows(y * s, s), :].astype(F32)
    for d in range(1, ny):
        own += ybuf[d].astype(F32)

    sq1[0] = jnp.sum(own * own, axis=0, keepdims=True)
    first = []
    for dy, dx in plane:
        k = dy * nx + dx
        to = {Y: wrap(y + dy, ny), X: wrap(x + dx, nx)}
        cp = remote(sq1.at[0], sq1.at[k], s1.at[k], r1.at[k], to)
        cp.start()
        first.append(cp)

    def slot(i):
        return rows(c * h + i * s, s)

    rall[slot(y), :] = own.astype(BF)
    gather = []
    for d in far_first(ny):
        cp = remote(rall.at[slot(y)], rall.at[slot(y)], ys2.at[d], yr2.at[d], {Y: wrap(y + d, ny)})
        cp.start()
        gather.append(cp)

    for cp in first:
        cp.wait()
    sq2[0] = jnp.sum(sq1[...], axis=0)
    second = []
    for dz, dc in line:
        k = dz * nc + dc
        to = {Z: wrap(z + dz, nz), C: wrap(c + dc, nc)}
        cp = remote(sq2.at[0], sq2.at[k], s2.at[k], r2.at[k], to)
        cp.start()
        second.append(cp)

    for d, cp in zip(far_first(ny), gather):
        cp.wait_send()
        src = wrap(y - d + ny, ny)
        remote(rall.at[slot(src)], rall.at[slot(src)], ys2.at[d], yr2.at[d], {Y: src}).wait_recv()
    mine = rows(c * h, h)
    cp = remote(rall.at[mine], rall.at[mine], cs2, cr2, peer)
    cp.start()
    cp.wait_send()
    other = rows((1 - c) * h, h)
    remote(rall.at[other], rall.at[other], cs2, cr2, peer).wait_recv()
    right_ref[...] = rall[...]
    for cp in second:
        cp.wait()
    colsq_ref[...] = jnp.sum(sq2[...], axis=0)


def vmem(n):
    return [pl.BlockSpec(memory_space=pltpu.VMEM)] * n


def per_device(sizes, weight, momentum, gradient, basis):
    nz, nx, ny, nc = sizes
    nloc, cols = momentum.shape
    q = nloc // nx
    th = 2 * q // nz
    h = RANK // 2
    dma = pltpu.SemaphoreType.DMA
    buft, power, gram = pl.pallas_call(
        functools.partial(power_kernel, sizes),
        out_shape=(
            jax.ShapeDtypeStruct((PAD, nloc), BF),
            jax.ShapeDtypeStruct((nloc, RANK), BF),
            jax.ShapeDtypeStruct((RANK, RANK), F32),
        ),
        in_specs=vmem(3),
        out_specs=tuple(vmem(3)),
        scratch_shapes=[
            pltpu.VMEM((nloc, PAD), BF),
            pltpu.VMEM((nloc, RANK), BF),
            pltpu.VMEM((nx, q, RANK), BF),
            pltpu.VMEM((q, RANK), BF),
            pltpu.VMEM((nz, th, 128), BF),
            pltpu.VMEM((nloc, RANK), BF),
            pltpu.VMEM((RANK, RANK), F32),
            pltpu.VMEM((h, RANK), F32),
            pltpu.VMEM((h, RANK), F32),
            pltpu.VMEM((ny, h // ny, RANK), F32),
            pltpu.VMEM((RANK, RANK), F32),
            dma((nx,)), dma((nx,)), dma((nz,)), dma((nz,)), dma((nz,)), dma((nz,)), dma((nx,)), dma((nx,)),
            dma, dma, dma((ny,)), dma((ny,)), dma((ny,)), dma((ny,)), dma, dma,
        ],
        compiler_params=pltpu.CompilerParams(collective_id=0, has_side_effects=True),
    )(momentum, gradient, basis)

    hi, lo = pl.pallas_call(
        factor_kernel,
        out_shape=(jax.ShapeDtypeStruct((RANK, RANK), BF),) * 2,
        in_specs=vmem(1),
        out_specs=tuple(vmem(2)),
        scratch_shapes=[pltpu.VMEM((RANK, RANK), F32)] * 2,
    )(gram)

    s = PAD // 2 // ny
    ortho, right, colsq = pl.pallas_call(
        functools.partial(right_kernel, sizes),
        out_shape=(
            jax.ShapeDtypeStruct((nloc, RANK), BF),
            jax.ShapeDtypeStruct((PAD, RANK), BF),
            jax.ShapeDtypeStruct((1, RANK), F32),
        ),
        in_specs=vmem(4),
        out_specs=tuple(vmem(3)),
        scratch_shapes=[
            pltpu.VMEM((PAD, RANK), BF),
            pltpu.VMEM((PAD // 2, RANK), BF),
            pltpu.VMEM((PAD // 2, RANK), BF),
            pltpu.VMEM((ny, s, RANK), BF),
            pltpu.VMEM((PAD, RANK), BF),
            pltpu.VMEM((ny * nx, 1, RANK), F32),
            pltpu.VMEM((nz * nc, 1, RANK), F32),
            dma, dma, dma((ny,)), dma((ny,)), dma((ny,)), dma((ny,)), dma, dma,
            dma((ny * nx,)), dma((ny * nx,)), dma((nz * nc,)), dma((nz * nc,)),
        ],
        compiler_params=pltpu.CompilerParams(collective_id=1, has_side_effects=True),
    )(power, hi, lo, buft)

    whole = right[:cols]
    buffer = (momentum.astype(F32) + gradient.astype(F32)).astype(BF)
    basis_new = (whole.astype(F32) / jnp.sqrt(colsq + 1e-06)).astype(BF)
    feedback = jnp.einsum("rk,ck->rc", ortho, whole, preferred_element_type=F32)
    momentum_new = (buffer.astype(F32) - 0.5 * feedback).astype(BF)
    coeff = 0.3 * (D * FF / RANK) ** 0.5 / 50.0
    update = jnp.einsum("rk,ck->rc", ortho, basis_new, preferred_element_type=F32)
    weight_new = (weight.astype(F32) - coeff * update).astype(BF)
    return (weight_new, momentum_new, basis_new)


def build(devices, sizes):
    finer = Mesh(devices.reshape(sizes), (Z, X, Y, C))
    return jax.shard_map(
        functools.partial(per_device, sizes),
        mesh=finer,
        in_specs=(P(ROW, FSDP), P(ROW, FSDP), P(ROW, FSDP), P(FSDP, None)),
        out_specs=(P(ROW, FSDP), P(ROW, FSDP), P(FSDP, None)),
        check_vma=False,
    )


def solution(mesh):
    return build(mesh.devices, SIZES)
```

```python
import functools

import jax
import jax.numpy as jnp
from jax import lax
from jax.experimental import pallas as pl
from jax.experimental.pallas import tpu as pltpu
from jax.sharding import Mesh
from jax.sharding import PartitionSpec as P

D = 8192
FF = 26624
RANK = 256
Z, X, Y, C = "fsdp_0", "fsdp_1", "row_0", "row_1"
FSDP = (Z, X)
ROW = (Y, C)
SIZES = (16, 4, 8, 2)
BF, F32 = jnp.bfloat16, jnp.float32
PAD = 512
MESH = pl.DeviceIdType.MESH


def far_first(n):
    return sorted(range(1, n), key=lambda d: -min(d, n - d))


def far_pairs(n, m):
    pairs = [(a, b) for a in range(n) for b in range(m) if a or b]
    return sorted(pairs, key=lambda p: -(min(p[0], n - p[0]) + min(p[1], m - p[1])))


def rows(start, size):
    return pl.ds(pl.multiple_of(start, size), size)


def wrap(i, n):
    return lax.rem(i, n)


def near_first(n):
    return far_first(n)[::-1]


def remote(src, dst, send, recv, peer):
    return pltpu.make_async_remote_copy(
        src_ref=src, dst_ref=dst, send_sem=send, recv_sem=recv, device_id=peer, device_id_type=MESH
    )


def power_kernel(
    sizes, m_ref, g_ref, b_ref, buft_ref, p_ref, gram_ref,
    mv, gv, bv, part, xbuf, zpart, zbuf, pbuf, gp, gbuf, gh, ybuf, gall,
    ins, xs, xr, zs, zr, zs2, zr2, xs2, xr2, cs, cr, ys, yr, ys2, yr2, cs2, cr2,
):
    nz, nx, ny, nc = sizes
    z, x, y, c = (lax.axis_index(a) for a in (Z, X, Y, C))
    loads = [pltpu.make_async_copy(a, b, ins.at[i]) for i, (a, b) in enumerate(((m_ref, mv), (g_ref, gv), (b_ref, bv)))]
    for cp in loads:
        cp.start()
    barrier = pltpu.get_barrier_semaphore()
    for axis, me, n in ((Z, z, nz), (X, x, nx), (Y, y, ny), (C, c, nc)):
        for d in far_first(n):
            pl.semaphore_signal(barrier, inc=1, device_id={axis: wrap(me + d, n)}, device_id_type=MESH)
    for cp in loads:
        cp.wait()

    buffer = (mv[...].astype(F32) + gv[...].astype(F32)).astype(BF)
    buft_ref[...] = buffer
    part[...] = lax.dot_general(
        bv[...], buffer, (((0,), (0,)), ((), ())), preferred_element_type=F32
    ).astype(BF)
    pl.semaphore_wait(barrier, nz + nx + ny + nc - 4)

    q = part.shape[1] // nx
    th = RANK // nz
    order = far_first(nz) + [0]

    def tile(i, j):
        return (rows(i * th, th), rows(j * q, q))

    scatter = {}
    for e in order:
        to = wrap(z + e, nz)
        for d in far_first(nx):
            peer = wrap(x + d, nx)
            k = e * nx + d
            cp = remote(part.at[tile(to, peer)], xbuf.at[k], xs.at[k], xr.at[k], {X: peer})
            cp.start()
            scatter[k] = cp

    second = {}
    for e in order:
        to = wrap(z + e, nz)
        total = part[tile(to, x)].astype(F32)
        for d in far_first(nx):
            scatter[e * nx + d].wait_recv()
            total += xbuf[e * nx + d].astype(F32)
        if e:
            zpart[e] = total.astype(BF)
            second[e] = remote(zpart.at[e], zbuf.at[e], zs.at[e], zr.at[e], {Z: to})
            second[e].start()
        else:
            own = total
    for e in near_first(nz):
        second[e].wait_recv()
        own += zbuf[e].astype(F32)

    def forward(i):
        t = pbuf.at[tile(i, x)]
        for d in far_first(nx):
            remote(t, t, xs2.at[d], xr2.at[d], {X: wrap(x + d, nx)}).start()

    pbuf[tile(z, x)] = own.astype(BF)
    home = pbuf.at[tile(z, x)]
    gather = []
    for d in far_first(nz):
        cp = remote(home, home, zs2.at[d], zr2.at[d], {Z: wrap(z + d, nz)})
        cp.start()
        gather.append(cp)
    forward(z)
    for cp in list(scatter.values()) + list(second.values()):
        cp.wait_send()
    for d in near_first(nz):
        src = wrap(z - d + nz, nz)
        there = pbuf.at[tile(src, x)]
        remote(there, there, zs2.at[d], zr2.at[d], {Z: src}).wait_recv()
        forward(src)
    for cp in gather:
        cp.wait_send()

    def quarter(j):
        return (pl.ds(0, RANK), rows(j * q, q))

    gp[...] = gram_of(pbuf[quarter(x)])
    for d in near_first(nx):
        src = wrap(x - d + nx, nx)
        there = pbuf.at[quarter(src)]
        remote(there, there, xs2.at[d], xr2.at[d], {X: src}).wait_recv()
        gp[...] += gram_of(pbuf[quarter(src)])

    h = RANK // 2
    peer = {C: 1 - c}
    cp = remote(gp.at[rows((1 - c) * h, h)], gbuf, cs, cr, peer)
    cp.start()
    for d in far_first(nx):
        mine = pbuf.at[quarter(x)]
        remote(mine, mine, xs2.at[d], xr2.at[d], {X: wrap(x + d, nx)}).wait_send()
    p_ref[...] = pbuf[...]
    cp.wait()
    gh[...] = gp[rows(c * h, h), :] + gbuf[...]

    s = h // ny
    copies = []
    for d in far_first(ny):
        to = wrap(y + d, ny)
        cp = remote(gh.at[rows(to * s, s)], ybuf.at[d], ys.at[d], yr.at[d], {Y: to})
        cp.start()
        copies.append(cp)
    for cp in copies:
        cp.wait()
    own = gh[rows(y * s, s), :]
    for d in range(1, ny):
        own += ybuf[d]

    def slot(i):
        return rows(c * h + i * s, s)

    def across(i):
        t = gall.at[slot(i)]
        remote(t, t, cs2, cr2, peer).start()

    gall[slot(y), :] = own
    copies = []
    for d in far_first(ny):
        cp = remote(gall.at[slot(y)], gall.at[slot(y)], ys2.at[d], yr2.at[d], {Y: wrap(y + d, ny)})
        cp.start()
        copies.append(cp)
    across(y)
    for d in near_first(ny):
        src = wrap(y - d + ny, ny)
        remote(gall.at[slot(src)], gall.at[slot(src)], ys2.at[d], yr2.at[d], {Y: src}).wait_recv()
        across(src)
    for cp in copies:
        cp.wait_send()
    half = rows(c * h, h)
    remote(gall.at[half], gall.at[half], cs2, cr2, peer).wait_send()
    other = rows((1 - c) * h, h)
    remote(gall.at[other], gall.at[other], cs2, cr2, peer).wait_recv()
    gram_ref[...] = gall[...]


def gram_of(block):
    return lax.dot_general(block, block, (((1,), (1,)), ((), ())), preferred_element_type=F32)


def full(a, b, dims):
    return lax.dot_general(
        a, b, (dims, ((), ())), precision=lax.Precision.HIGHEST, preferred_element_type=F32
    )


def quick(a, b, dims):
    return lax.dot_general(a.astype(BF), b.astype(BF), (dims, ((), ())), preferred_element_type=F32)


def newton_step(product, sym, low):
    n = RANK
    i = lax.broadcasted_iota(jnp.int32, (n, n), 0)
    j = lax.broadcasted_iota(jnp.int32, (n, n), 1)
    inv = low[...]
    e = product(product(inv, sym[...], ((1,), (0,))), inv, ((1,), (1,)))
    e = e - jnp.where(i == j, 1.0, 0.0)
    phi = jnp.where(i > j, e, jnp.where(i == j, 0.5 * e, 0.0))
    low[...] = inv - product(phi, inv, ((1,), (0,)))
    return jnp.sum(e * e)


def factor_kernel(g_ref, sym, low, scale_ref, work):
    n = RANK
    i = lax.broadcasted_iota(jnp.int32, (n, n), 0)
    j = lax.broadcasted_iota(jnp.int32, (n, n), 1)
    gram = g_ref[...]
    diag = jnp.where(i == j, gram, 0.0)
    across = lax.rsqrt(jnp.sum(diag, axis=0, keepdims=True))
    down = lax.rsqrt(jnp.sum(diag, axis=1, keepdims=True))
    scale_ref[...] = across
    normed = gram * across * down
    sym[...] = normed
    low[...] = jnp.where(i > j, -normed, jnp.where(i == j, 1.5 - 0.5 * normed, 0.0))
    small = 1e-2

    def more(state):
        step, err = state
        return jnp.logical_and(step < 12, err > small)

    def newton(state):
        return state[0] + 1, newton_step(quick, sym, low)

    _, err = lax.while_loop(more, newton, (0, jnp.float32(1.0)))

    @pl.when(jnp.logical_not(err <= small))
    def _():
        work[...] = sym[...]
        low[...] = jnp.where(i == j, 1.0, 0.0)
        lane = lax.broadcasted_iota(jnp.int32, (1, n), 1)
        line = lax.broadcasted_iota(jnp.int32, (n, 1), 0)

        def column(k, _):
            pivots = work[pl.ds(k, 1), :]
            pivot = jnp.sum(jnp.where(lane == k, pivots, 0.0), axis=1, keepdims=True)
            inverse = low[pl.ds(k, 1), :]
            here = work[...]
            col = jnp.sum(jnp.where(j == k, here, 0.0), axis=1, keepdims=True)
            times = jnp.where(line > k, col / pivot, 0.0)
            work[...] = here - times * pivots
            low[...] = low[...] - times * inverse
            return 0

        lax.fori_loop(0, n, column, 0)
        pivot = jnp.sum(jnp.where(i == j, work[...], 0.0), axis=1, keepdims=True)
        low[...] = low[...] * lax.rsqrt(pivot)


def right_kernel(
    sizes, p_ref, sym, low_ref, scale_ref, buft_ref, w_ref,
    ortho_ref, right_ref, colsq_ref, mom_ref, wout_ref,
    low, part, cbuf, half, ybuf, rall, sq1, sq2,
    ins, cs, cr, ys, yr, ys2, yr2, cs2, cr2, s1, r1, s2, r2,
):
    nz, nx, ny, nc = sizes
    z, x, y, c = (lax.axis_index(a) for a in (Z, X, Y, C))
    barrier = pltpu.get_barrier_semaphore()
    plane = far_pairs(ny, nx)
    line = far_pairs(nz, nc)
    for dz, dc in line:
        to = {Z: wrap(z + dz, nz), C: wrap(c + dc, nc)}
        pl.semaphore_signal(barrier, inc=1, device_id=to, device_id_type=MESH)
    for dy, dx in plane:
        to = {Y: wrap(y + dy, ny), X: wrap(x + dx, nx)}
        pl.semaphore_signal(barrier, inc=1, device_id=to, device_id_type=MESH)
    load = pltpu.make_async_copy(w_ref, wout_ref, ins)
    load.start()

    low[...] = low_ref[...]
    for _ in range(2):
        newton_step(full, sym, low)
    inv = low[...] * scale_ref[...]
    hi = inv.astype(BF)
    lo = (inv - hi.astype(F32)).astype(BF)
    power = p_ref[...]
    ortho = jnp.dot(hi, power, preferred_element_type=F32)
    ortho += jnp.dot(lo, power, preferred_element_type=F32)
    ortho = ortho.astype(BF)
    ortho_ref[...] = ortho
    cols = buft_ref.shape[0]
    part[:cols, :] = lax.dot_general(
        buft_ref[...], ortho, (((1,), (1,)), ((), ())), preferred_element_type=F32
    ).astype(BF)
    part[cols:, :] = jnp.zeros((PAD - cols, RANK), BF)
    pl.semaphore_wait(barrier, len(plane) + len(line))

    h = PAD // 2
    peer = {C: 1 - c}
    cp = remote(part.at[rows((1 - c) * h, h)], cbuf, cs, cr, peer)
    cp.start()
    cp.wait()
    half[...] = (part[rows(c * h, h), :].astype(F32) + cbuf[...].astype(F32)).astype(BF)

    s = h // ny
    copies = []
    for d in far_first(ny):
        to = wrap(y + d, ny)
        cp = remote(half.at[rows(to * s, s)], ybuf.at[d], ys.at[d], yr.at[d], {Y: to})
        cp.start()
        copies.append(cp)
    for cp in copies:
        cp.wait()
    own = half[rows(y * s, s), :].astype(F32)
    for d in range(1, ny):
        own += ybuf[d].astype(F32)

    sq1[0] = jnp.sum(own * own, axis=0, keepdims=True)
    first = []
    for dy, dx in plane:
        k = dy * nx + dx
        to = {Y: wrap(y + dy, ny), X: wrap(x + dx, nx)}
        cp = remote(sq1.at[0], sq1.at[k], s1.at[k], r1.at[k], to)
        cp.start()
        first.append(cp)

    def slot(i):
        return rows(c * h + i * s, s)

    rall[slot(y), :] = own.astype(BF)
    gather = []
    for d in far_first(ny):
        cp = remote(rall.at[slot(y)], rall.at[slot(y)], ys2.at[d], yr2.at[d], {Y: wrap(y + d, ny)})
        cp.start()
        gather.append(cp)

    for cp in first:
        cp.wait()
    sq2[0] = jnp.sum(sq1[...], axis=0)
    second = []
    for dz, dc in line:
        k = dz * nc + dc
        to = {Z: wrap(z + dz, nz), C: wrap(c + dc, nc)}
        cp = remote(sq2.at[0], sq2.at[k], s2.at[k], r2.at[k], to)
        cp.start()
        second.append(cp)

    for d, cp in zip(far_first(ny), gather):
        cp.wait_send()
        src = wrap(y - d + ny, ny)
        remote(rall.at[slot(src)], rall.at[slot(src)], ys2.at[d], yr2.at[d], {Y: src}).wait_recv()
    mine = rows(c * h, h)
    cp = remote(rall.at[mine], rall.at[mine], cs2, cr2, peer)
    cp.start()
    cp.wait_send()
    other = rows((1 - c) * h, h)
    remote(rall.at[other], rall.at[other], cs2, cr2, peer).wait_recv()
    right_ref[...] = rall[...]
    feedback = jnp.dot(rall[:cols, :], ortho_ref[...], preferred_element_type=F32)
    mom_ref[...] = (buft_ref[...].astype(F32) - 0.5 * feedback).astype(BF)
    load.wait()
    for cp in second:
        cp.wait()
    colsq_ref[...] = jnp.sum(sq2[...], axis=0)


def update_kernel(
    ortho_ref, right_ref, colsq_ref, mom_ref, w_ref, weight_ref, momentum_ref, basis_ref, wv, bv, outs
):
    first = pltpu.make_async_copy(mom_ref, momentum_ref, outs.at[0])
    first.start()
    cols = wv.shape[0]
    length = jnp.sqrt(colsq_ref[...] + 1e-06)
    basis = (right_ref[:cols, :].astype(F32) / length).astype(BF)
    bv[...] = basis
    second = pltpu.make_async_copy(bv, basis_ref, outs.at[1])
    second.start()
    coeff = 0.3 * (D * FF / RANK) ** 0.5 / 50.0
    update = jnp.dot(basis, ortho_ref[...], preferred_element_type=F32)
    wv[...] = (w_ref[...].astype(F32) - coeff * update).astype(BF)
    third = pltpu.make_async_copy(wv, weight_ref, outs.at[2])
    third.start()
    for cp in (first, second, third):
        cp.wait()


def vmem(n):
    return [pl.BlockSpec(memory_space=pltpu.VMEM)] * n


def anywhere(n):
    return [pl.BlockSpec(memory_space=pl.ANY)] * n


def bf(*shape):
    return jax.ShapeDtypeStruct(shape, BF)


def f32(*shape):
    return jax.ShapeDtypeStruct(shape, F32)


def per_device(sizes, weight, momentum, gradient, basis):
    nz, nx, ny, nc = sizes
    nloc, cols = momentum.shape
    q = nloc // nx
    th = RANK // nz
    h = RANK // 2
    dma = pltpu.SemaphoreType.DMA
    buft, power, gram = pl.pallas_call(
        functools.partial(power_kernel, sizes),
        out_shape=(bf(cols, nloc), bf(RANK, nloc), f32(RANK, RANK)),
        in_specs=anywhere(3),
        out_specs=tuple(vmem(3)),
        scratch_shapes=[
            pltpu.VMEM((cols, nloc), BF),
            pltpu.VMEM((cols, nloc), BF),
            pltpu.VMEM((cols, RANK), BF),
            pltpu.VMEM((RANK, nloc), BF),
            pltpu.VMEM((nx * nz, th, q), BF),
            pltpu.VMEM((nz, th, q), BF),
            pltpu.VMEM((nz, th, q), BF),
            pltpu.VMEM((RANK, nloc), BF),
            pltpu.VMEM((RANK, RANK), F32),
            pltpu.VMEM((h, RANK), F32),
            pltpu.VMEM((h, RANK), F32),
            pltpu.VMEM((ny, h // ny, RANK), F32),
            pltpu.VMEM((RANK, RANK), F32),
            dma((3,)), dma((nx * nz,)), dma((nx * nz,)),
            dma((nz,)), dma((nz,)), dma((nz,)), dma((nz,)), dma((nx,)), dma((nx,)),
            dma, dma, dma((ny,)), dma((ny,)), dma((ny,)), dma((ny,)), dma, dma,
        ],
        compiler_params=pltpu.CompilerParams(collective_id=0, has_side_effects=True),
    )(momentum.T, gradient.T, basis)

    sym, low, scale = pl.pallas_call(
        factor_kernel,
        out_shape=(f32(RANK, RANK), f32(RANK, RANK), f32(1, RANK)),
        in_specs=vmem(1),
        out_specs=tuple(vmem(3)),
        scratch_shapes=[pltpu.VMEM((RANK, RANK), F32)],
    )(gram)

    s = PAD // 2 // ny
    ortho, right, colsq, mom, held = pl.pallas_call(
        functools.partial(right_kernel, sizes),
        out_shape=(bf(RANK, nloc), bf(PAD, RANK), f32(1, RANK), bf(cols, nloc), bf(cols, nloc)),
        in_specs=vmem(5) + anywhere(1),
        out_specs=tuple(vmem(5)),
        scratch_shapes=[
            pltpu.VMEM((RANK, RANK), F32),
            pltpu.VMEM((PAD, RANK), BF),
            pltpu.VMEM((PAD // 2, RANK), BF),
            pltpu.VMEM((PAD // 2, RANK), BF),
            pltpu.VMEM((ny, s, RANK), BF),
            pltpu.VMEM((PAD, RANK), BF),
            pltpu.VMEM((ny * nx, 1, RANK), F32),
            pltpu.VMEM((nz * nc, 1, RANK), F32),
            dma, dma, dma, dma((ny,)), dma((ny,)), dma((ny,)), dma((ny,)), dma, dma,
            dma((ny * nx,)), dma((ny * nx,)), dma((nz * nc,)), dma((nz * nc,)),
        ],
        compiler_params=pltpu.CompilerParams(collective_id=1, has_side_effects=True),
    )(power, sym, low, scale, buft, weight.T)

    weight_new, momentum_new, basis_new = pl.pallas_call(
        update_kernel,
        out_shape=(bf(cols, nloc), bf(cols, nloc), bf(cols, RANK)),
        in_specs=vmem(5),
        out_specs=tuple(anywhere(3)),
        scratch_shapes=[pltpu.VMEM((cols, nloc), BF), pltpu.VMEM((cols, RANK), BF), dma((3,))],
    )(ortho, right, colsq, mom, held)
    return weight_new.T, momentum_new.T, basis_new


def build(devices, sizes):
    finer = Mesh(devices.reshape(sizes), (Z, X, Y, C))
    return jax.shard_map(
        functools.partial(per_device, sizes),
        mesh=finer,
        in_specs=(P(ROW, FSDP), P(ROW, FSDP), P(ROW, FSDP), P(FSDP, None)),
        out_specs=(P(ROW, FSDP), P(ROW, FSDP), P(FSDP, None)),
        check_vma=False,
    )


def solution(mesh):
    return build(mesh.devices, SIZES)
```

```python
import functools

import jax
import jax.numpy as jnp
from jax import lax
from jax.experimental import pallas as pl
from jax.experimental.pallas import tpu as pltpu
from jax.sharding import Mesh
from jax.sharding import PartitionSpec as P

D = 8192
FF = 26624
RANK = 256
Z, X, Y, C = "fsdp_0", "fsdp_1", "row_0", "row_1"
FSDP = (Z, X)
ROW = (Y, C)
SIZES = (16, 4, 8, 2)
BF, F32 = jnp.bfloat16, jnp.float32
PAD = 512
SMALL = 1e-2
MESH = pl.DeviceIdType.MESH


def far_first(n):
    return sorted(range(1, n), key=lambda d: -min(d, n - d))


def far_pairs(n, m):
    pairs = [(a, b) for a in range(n) for b in range(m) if a or b]
    return sorted(pairs, key=lambda p: -(min(p[0], n - p[0]) + min(p[1], m - p[1])))


def rows(start, size):
    return pl.ds(pl.multiple_of(start, size), size)


def wrap(i, n):
    return lax.rem(i, n)


def near_first(n):
    return far_first(n)[::-1]


def remote(src, dst, send, recv, peer):
    return pltpu.make_async_remote_copy(
        src_ref=src, dst_ref=dst, send_sem=send, recv_sem=recv, device_id=peer, device_id_type=MESH
    )


def lanes(a, b):
    return lax.dot_general(a, b, (((1,), (1,)), ((), ())), preferred_element_type=F32)


def full(a, b, dims):
    return lax.dot_general(
        a, b, (dims, ((), ())), precision=lax.Precision.HIGHEST, preferred_element_type=F32
    )


def quick(a, b, dims):
    return lax.dot_general(a.astype(BF), b.astype(BF), (dims, ((), ())), preferred_element_type=F32)


def square():
    n = RANK
    return (lax.broadcasted_iota(jnp.int32, (n, n), axis) for axis in (0, 1))


def newton_step(product, sym, low):
    i, j = square()
    inv = low[...]
    e = product(product(inv, sym[...], ((1,), (0,))), inv, ((1,), (1,)))
    e = e - jnp.where(i == j, 1.0, 0.0)
    phi = jnp.where(i > j, e, jnp.where(i == j, 0.5 * e, 0.0))
    low[...] = inv - product(phi, inv, ((1,), (0,)))
    return jnp.sum(e * e)


def fast_kernel(
    sizes, m_ref, g_ref, b_ref,
    buft_ref, p_ref, gram_ref, ortho_ref, right_ref, mom_ref, colsq_ref, err_ref,
    mv, gv, bv, buft, part, xbuf, zpart, zbuf, pbuf, gp, gbuf, gh, ybuf, gall, sym, low,
    obuf, rpart, cbuf, rhalf, wbuf, rall, sq1, sq2, mom,
    ins, store, xs, xr, zs, zr, zs2, zr2, xs2, xr2, cs, cr, ys, yr, ys2, yr2, cs2, cr2,
    cs3, cr3, ys3, yr3, ys4, yr4, cs4, cr4, s1, r1, s2, r2,
):
    nz, nx, ny, nc = sizes
    z, x, y, c = (lax.axis_index(a) for a in (Z, X, Y, C))
    loads = [pltpu.make_async_copy(a, b, ins.at[i]) for i, (a, b) in enumerate(((m_ref, mv), (g_ref, gv), (b_ref, bv)))]
    for cp in loads:
        cp.start()
    barrier = pltpu.get_barrier_semaphore()
    plane = far_pairs(ny, nx)
    line = far_pairs(nz, nc)
    for dz, dc in line:
        to = {Z: wrap(z + dz, nz), C: wrap(c + dc, nc)}
        pl.semaphore_signal(barrier, inc=1, device_id=to, device_id_type=MESH)
    for dy, dx in plane:
        to = {Y: wrap(y + dy, ny), X: wrap(x + dx, nx)}
        pl.semaphore_signal(barrier, inc=1, device_id=to, device_id_type=MESH)
    for cp in loads:
        cp.wait()

    buffer = (mv[...].astype(F32) + gv[...].astype(F32)).astype(BF)
    buft[...] = buffer
    part[...] = lax.dot_general(
        bv[...], buffer, (((0,), (0,)), ((), ())), preferred_element_type=F32
    ).astype(BF)
    outs = [pltpu.make_async_copy(buft, buft_ref, store.at[0])]
    outs[0].start()
    pl.semaphore_wait(barrier, len(plane) + len(line))

    q = part.shape[1] // nx
    th = RANK // nz
    order = far_first(nz) + [0]

    def tile(i, j):
        return (rows(i * th, th), rows(j * q, q))

    scatter = {}
    for e in order:
        to = wrap(z + e, nz)
        for d in far_first(nx):
            peer = wrap(x + d, nx)
            k = e * nx + d
            cp = remote(part.at[tile(to, peer)], xbuf.at[k], xs.at[k], xr.at[k], {X: peer})
            cp.start()
            scatter[k] = cp

    second = {}
    for e in order:
        to = wrap(z + e, nz)
        total = part[tile(to, x)].astype(F32)
        for d in far_first(nx):
            scatter[e * nx + d].wait_recv()
            total += xbuf[e * nx + d].astype(F32)
        if e:
            zpart[e] = total.astype(BF)
            second[e] = remote(zpart.at[e], zbuf.at[e], zs.at[e], zr.at[e], {Z: to})
            second[e].start()
        else:
            own = total
    for e in near_first(nz):
        second[e].wait_recv()
        own += zbuf[e].astype(F32)

    def forward(i):
        t = pbuf.at[tile(i, x)]
        for d in far_first(nx):
            remote(t, t, xs2.at[d], xr2.at[d], {X: wrap(x + d, nx)}).start()

    pbuf[tile(z, x)] = own.astype(BF)
    home = pbuf.at[tile(z, x)]
    gather = []
    for d in far_first(nz):
        cp = remote(home, home, zs2.at[d], zr2.at[d], {Z: wrap(z + d, nz)})
        cp.start()
        gather.append(cp)
    forward(z)
    for cp in list(scatter.values()) + list(second.values()):
        cp.wait_send()
    for d in near_first(nz):
        src = wrap(z - d + nz, nz)
        there = pbuf.at[tile(src, x)]
        remote(there, there, zs2.at[d], zr2.at[d], {Z: src}).wait_recv()
        forward(src)
    for cp in gather:
        cp.wait_send()

    def quarter(j):
        return (pl.ds(0, RANK), rows(j * q, q))

    for d in near_first(nx):
        src = wrap(x - d + nx, nx)
        there = pbuf.at[quarter(src)]
        remote(there, there, xs2.at[d], xr2.at[d], {X: src}).wait_recv()
    outs.append(pltpu.make_async_copy(pbuf, p_ref, store.at[1]))
    outs[1].start()
    b = RANK // 2
    gp[: 2 * b, :] = lanes(pbuf[...], pbuf[:b, :])
    gp[2 * b :, :] = lanes(pbuf[b:, :], pbuf[b:, :])

    h = 3 * b // 2
    peer = {C: 1 - c}
    cp = remote(gp.at[rows((1 - c) * h, h)], gbuf, cs, cr, peer)
    cp.start()
    for d in far_first(nx):
        mine = pbuf.at[quarter(x)]
        remote(mine, mine, xs2.at[d], xr2.at[d], {X: wrap(x + d, nx)}).wait_send()
    cp.wait()
    gh[...] = gp[rows(c * h, h), :] + gbuf[...]

    s = h // ny
    copies = []
    for d in far_first(ny):
        to = wrap(y + d, ny)
        cp = remote(gh.at[rows(to * s, s)], ybuf.at[d], ys.at[d], yr.at[d], {Y: to})
        cp.start()
        copies.append(cp)
    for cp in copies:
        cp.wait()
    own = gh[rows(y * s, s), :]
    for d in range(1, ny):
        own += ybuf[d]

    def slot(i):
        return rows(c * h + i * s, s)

    def across(i):
        t = gall.at[slot(i)]
        remote(t, t, cs2, cr2, peer).start()

    gall[slot(y), :] = own
    copies = []
    for d in far_first(ny):
        cp = remote(gall.at[slot(y)], gall.at[slot(y)], ys2.at[d], yr2.at[d], {Y: wrap(y + d, ny)})
        cp.start()
        copies.append(cp)
    across(y)
    for d in near_first(ny):
        src = wrap(y - d + ny, ny)
        remote(gall.at[slot(src)], gall.at[slot(src)], ys2.at[d], yr2.at[d], {Y: src}).wait_recv()
        across(src)
    for cp in copies:
        cp.wait_send()
    half = rows(c * h, h)
    remote(gall.at[half], gall.at[half], cs2, cr2, peer).wait_send()
    other = rows((1 - c) * h, h)
    remote(gall.at[other], gall.at[other], cs2, cr2, peer).wait_recv()
    outs.append(pltpu.make_async_copy(gall, gram_ref, store.at[2]))
    outs[2].start()

    corner = gall[b : 2 * b, :]
    sym[:b, :b] = gall[:b, :]
    sym[b:, :b] = corner
    sym[:b, b:] = corner.T
    sym[b:, b:] = gall[2 * b :, :]
    gram = sym[...]
    i, j = square()
    diag = jnp.where(i == j, gram, 0.0)
    scale = lax.rsqrt(jnp.sum(diag, axis=0, keepdims=True))
    down = lax.rsqrt(jnp.sum(diag, axis=1, keepdims=True))
    normed = gram * scale * down
    sym[...] = normed
    low[...] = jnp.where(i > j, -normed, jnp.where(i == j, 1.5 - 0.5 * normed, 0.0))
    newton_step(quick, sym, low)
    err_ref[...] = jnp.zeros((1, 128), F32) + newton_step(full, sym, low)
    inv = low[...] * scale
    hi = inv.astype(BF)
    lo = (inv - hi.astype(F32)).astype(BF)
    power = pbuf[...]
    ortho = jnp.dot(hi, power, preferred_element_type=F32)
    ortho += jnp.dot(lo, power, preferred_element_type=F32)
    ortho = ortho.astype(BF)
    obuf[...] = ortho
    outs.append(pltpu.make_async_copy(obuf, ortho_ref, store.at[3]))
    outs[3].start()
    cols = buft.shape[0]
    rpart[:cols, :] = lanes(buft[...], ortho).astype(BF)
    rpart[cols:, :] = jnp.zeros((PAD - cols, RANK), BF)

    h = PAD // 2
    peer = {C: 1 - c}
    cp = remote(rpart.at[rows((1 - c) * h, h)], cbuf, cs3, cr3, peer)
    cp.start()
    cp.wait()
    rhalf[...] = (rpart[rows(c * h, h), :].astype(F32) + cbuf[...].astype(F32)).astype(BF)

    s = h // ny
    copies = []
    for d in far_first(ny):
        to = wrap(y + d, ny)
        cp = remote(rhalf.at[rows(to * s, s)], wbuf.at[d], ys3.at[d], yr3.at[d], {Y: to})
        cp.start()
        copies.append(cp)
    for cp in copies:
        cp.wait()
    own = rhalf[rows(y * s, s), :].astype(F32)
    for d in range(1, ny):
        own += wbuf[d].astype(F32)

    sq1[0] = jnp.sum(own * own, axis=0, keepdims=True)
    first = []
    for dy, dx in plane:
        k = dy * nx + dx
        to = {Y: wrap(y + dy, ny), X: wrap(x + dx, nx)}
        cp = remote(sq1.at[0], sq1.at[k], s1.at[k], r1.at[k], to)
        cp.start()
        first.append(cp)

    def slot(i):
        return rows(c * h + i * s, s)

    rall[slot(y), :] = own.astype(BF)
    gather = []
    for d in far_first(ny):
        cp = remote(rall.at[slot(y)], rall.at[slot(y)], ys4.at[d], yr4.at[d], {Y: wrap(y + d, ny)})
        cp.start()
        gather.append(cp)

    for cp in first:
        cp.wait()
    sq2[0] = jnp.sum(sq1[...], axis=0)
    second = []
    for dz, dc in line:
        k = dz * nc + dc
        to = {Z: wrap(z + dz, nz), C: wrap(c + dc, nc)}
        cp = remote(sq2.at[0], sq2.at[k], s2.at[k], r2.at[k], to)
        cp.start()
        second.append(cp)

    for d, cp in zip(far_first(ny), gather):
        cp.wait_send()
        src = wrap(y - d + ny, ny)
        remote(rall.at[slot(src)], rall.at[slot(src)], ys4.at[d], yr4.at[d], {Y: src}).wait_recv()
    mine = rows(c * h, h)
    cp = remote(rall.at[mine], rall.at[mine], cs4, cr4, peer)
    cp.start()
    cp.wait_send()
    other = rows((1 - c) * h, h)
    remote(rall.at[other], rall.at[other], cs4, cr4, peer).wait_recv()
    outs.append(pltpu.make_async_copy(rall, right_ref, store.at[4]))
    outs[4].start()
    feedback = jnp.dot(rall[:cols, :], ortho, preferred_element_type=F32)
    mom[...] = (buft[...].astype(F32) - 0.5 * feedback).astype(BF)
    outs.append(pltpu.make_async_copy(mom, mom_ref, store.at[5]))
    outs[5].start()
    for cp in second:
        cp.wait()
    colsq_ref[...] = jnp.sum(sq2[...], axis=0)
    for cp in outs:
        cp.wait()


def direct_kernel(g_ref, inv_ref, work):
    n = RANK
    i, j = square()
    gram = g_ref[...]
    diag = jnp.where(i == j, gram, 0.0)
    across = lax.rsqrt(jnp.sum(diag, axis=0, keepdims=True))
    down = lax.rsqrt(jnp.sum(diag, axis=1, keepdims=True))
    work[...] = gram * across * down
    inv_ref[...] = jnp.where(i == j, 1.0, 0.0)
    lane = lax.broadcasted_iota(jnp.int32, (1, n), 1)
    line = lax.broadcasted_iota(jnp.int32, (n, 1), 0)

    def column(k, _):
        pivots = work[pl.ds(k, 1), :]
        pivot = jnp.sum(jnp.where(lane == k, pivots, 0.0), axis=1, keepdims=True)
        inverse = inv_ref[pl.ds(k, 1), :]
        here = work[...]
        col = jnp.sum(jnp.where(j == k, here, 0.0), axis=1, keepdims=True)
        times = jnp.where(line > k, col / pivot, 0.0)
        work[...] = here - times * pivots
        inv_ref[...] = inv_ref[...] - times * inverse
        return 0

    lax.fori_loop(0, n, column, 0)
    pivot = jnp.sum(jnp.where(i == j, work[...], 0.0), axis=1, keepdims=True)
    inv_ref[...] = inv_ref[...] * lax.rsqrt(pivot) * across


def update_kernel(
    ortho_ref, right_ref, colsq_ref, mom_ref, w_ref, weight_ref, momentum_ref, basis_ref, wv, bv, outs
):
    first = pltpu.make_async_copy(mom_ref, momentum_ref, outs.at[0])
    first.start()
    cols = wv.shape[0]
    length = jnp.sqrt(colsq_ref[...] + 1e-06)
    basis = (right_ref[:cols, :].astype(F32) / length).astype(BF)
    bv[...] = basis
    second = pltpu.make_async_copy(bv, basis_ref, outs.at[1])
    second.start()
    coeff = 0.3 * (D * FF / RANK) ** 0.5 / 50.0
    update = jnp.dot(basis, ortho_ref[...], preferred_element_type=F32)
    wv[...] = (w_ref[...].astype(F32) - coeff * update).astype(BF)
    third = pltpu.make_async_copy(wv, weight_ref, outs.at[2])
    third.start()
    for cp in (first, second, third):
        cp.wait()


def vmem(n):
    return [pl.BlockSpec(memory_space=pltpu.VMEM)] * n


def anywhere(n):
    return [pl.BlockSpec(memory_space=pl.ANY)] * n


def bf(*shape):
    return jax.ShapeDtypeStruct(shape, BF)


def f32(*shape):
    return jax.ShapeDtypeStruct(shape, F32)


def finish(ortho, right, colsq, mom, weight):
    cols, nloc = mom.shape
    return pl.pallas_call(
        update_kernel,
        out_shape=(bf(cols, nloc), bf(cols, nloc), bf(cols, RANK)),
        in_specs=vmem(5),
        out_specs=tuple(anywhere(3)),
        scratch_shapes=[pltpu.VMEM((cols, nloc), BF), pltpu.VMEM((cols, RANK), BF), pltpu.SemaphoreType.DMA((3,))],
    )(ortho, right, colsq, mom, weight)


def general(sizes, buft, power, gram, weight):
    b = RANK // 2
    corner = gram[b : 2 * b]
    upper = jnp.concatenate([gram[:b], corner.T], axis=1)
    lower = jnp.concatenate([corner, gram[2 * b :]], axis=1)
    inv = pl.pallas_call(
        direct_kernel,
        out_shape=f32(RANK, RANK),
        in_specs=vmem(1),
        out_specs=vmem(1)[0],
        scratch_shapes=[pltpu.VMEM((RANK, RANK), F32)],
    )(jnp.concatenate([upper, lower]))
    hi = inv.astype(BF)
    lo = (inv - hi.astype(F32)).astype(BF)
    ortho = jnp.dot(hi, power, preferred_element_type=F32)
    ortho = (ortho + jnp.dot(lo, power, preferred_element_type=F32)).astype(BF)
    right = jnp.einsum("cr,kr->ck", buft, ortho, preferred_element_type=F32)
    pieces = right.reshape(sizes[2] * sizes[3], -1, RANK)
    share = jnp.sum(lax.all_to_all(pieces, ROW, 0, 0, tiled=True), axis=0)
    whole = lax.all_gather(share.astype(BF), ROW, tiled=True)
    colsq = jnp.sum(share * share, axis=0, keepdims=True)
    colsq = jnp.sum(lax.all_gather(colsq, ROW, tiled=True), axis=0, keepdims=True)
    colsq = jnp.sum(lax.all_gather(colsq, FSDP, tiled=True), axis=0, keepdims=True)
    feedback = jnp.dot(whole, ortho, preferred_element_type=F32)
    mom = (buft.astype(F32) - 0.5 * feedback).astype(BF)
    whole = jnp.pad(whole, ((0, PAD - whole.shape[0]), (0, 0)))
    return finish(ortho, whole, colsq, mom, weight)


def per_device(sizes, weight, momentum, gradient, basis):
    nz, nx, ny, nc = sizes
    nloc, cols = momentum.shape
    q = nloc // nx
    th = RANK // nz
    b = RANK // 2
    h = 3 * b // 2
    s = PAD // 2 // ny
    dma = pltpu.SemaphoreType.DMA
    scratch = [
        bf(cols, nloc), bf(cols, nloc), bf(cols, RANK), bf(cols, nloc), bf(RANK, nloc),
        bf(nx * nz, th, q), bf(nz, th, q), bf(nz, th, q), bf(RANK, nloc),
        f32(3 * b, b), f32(h, b), f32(h, b), f32(ny, h // ny, b), f32(3 * b, b), f32(RANK, RANK), f32(RANK, RANK),
        bf(RANK, nloc), bf(PAD, RANK), bf(PAD // 2, RANK), bf(PAD // 2, RANK), bf(ny, s, RANK), bf(PAD, RANK),
        f32(ny * nx, 1, RANK), f32(nz * nc, 1, RANK), bf(cols, nloc),
    ]
    buft, power, gram, ortho, right, mom, colsq, err = pl.pallas_call(
        functools.partial(fast_kernel, sizes),
        out_shape=(
            bf(cols, nloc), bf(RANK, nloc), f32(3 * b, b), bf(RANK, nloc), bf(PAD, RANK), bf(cols, nloc),
            f32(1, RANK), f32(1, 128),
        ),
        in_specs=anywhere(3),
        out_specs=tuple(anywhere(6) + vmem(2)),
        scratch_shapes=[pltpu.VMEM(v.shape, v.dtype) for v in scratch] + [
            dma((3,)), dma((6,)), dma((nx * nz,)), dma((nx * nz,)),
            dma((nz,)), dma((nz,)), dma((nz,)), dma((nz,)), dma((nx,)), dma((nx,)),
            dma, dma, dma((ny,)), dma((ny,)), dma((ny,)), dma((ny,)), dma, dma,
            dma, dma, dma((ny,)), dma((ny,)), dma((ny,)), dma((ny,)), dma, dma,
            dma((ny * nx,)), dma((ny * nx,)), dma((nz * nc,)), dma((nz * nc,)),
        ],
        compiler_params=pltpu.CompilerParams(collective_id=0, has_side_effects=True),
    )(momentum.T, gradient.T, basis)

    weight_new, momentum_new, basis_new = lax.cond(
        err[0, 0] <= SMALL,
        lambda: finish(ortho, right, colsq, mom, weight.T),
        lambda: general(sizes, buft, power, gram, weight.T),
    )
    return weight_new.T, momentum_new.T, basis_new


def build(devices, sizes):
    finer = Mesh(devices.reshape(sizes), (Z, X, Y, C))
    return jax.shard_map(
        functools.partial(per_device, sizes),
        mesh=finer,
        in_specs=(P(ROW, FSDP), P(ROW, FSDP), P(ROW, FSDP), P(FSDP, None)),
        out_specs=(P(ROW, FSDP), P(ROW, FSDP), P(FSDP, None)),
        check_vma=False,
    )


def solution(mesh):
    return build(mesh.devices, SIZES)
```

```python
import functools

import jax
import jax.numpy as jnp
from jax import lax
from jax.experimental import pallas as pl
from jax.experimental.pallas import tpu as pltpu
from jax.sharding import Mesh
from jax.sharding import PartitionSpec as P

D = 8192
FF = 26624
RANK = 256
Z, X, Y, C = "fsdp_0", "fsdp_1", "row_0", "row_1"
FSDP = (Z, X)
ROW = (Y, C)
SIZES = (16, 4, 8, 2)
BF, F32 = jnp.bfloat16, jnp.float32
PAD = 512
SMALL = 1e-2
MESH = pl.DeviceIdType.MESH


def far_first(n):
    return sorted(range(1, n), key=lambda d: -min(d, n - d))


def far_pairs(n, m):
    pairs = [(a, b) for a in range(n) for b in range(m) if a or b]
    return sorted(pairs, key=lambda p: -(min(p[0], n - p[0]) + min(p[1], m - p[1])))


def rows(start, size):
    return pl.ds(pl.multiple_of(start, size), size)


def wrap(i, n):
    return lax.rem(i, n)


def near_first(n):
    return far_first(n)[::-1]


def remote(src, dst, send, recv, peer):
    return pltpu.make_async_remote_copy(
        src_ref=src, dst_ref=dst, send_sem=send, recv_sem=recv, device_id=peer, device_id_type=MESH
    )


def lanes(a, b):
    return lax.dot_general(a, b, (((1,), (1,)), ((), ())), preferred_element_type=F32)


def full(a, b, dims):
    return lax.dot_general(
        a, b, (dims, ((), ())), precision=lax.Precision.HIGHEST, preferred_element_type=F32
    )


def quick(a, b, dims):
    return lax.dot_general(a.astype(BF), b.astype(BF), (dims, ((), ())), preferred_element_type=F32)


def square():
    n = RANK
    return (lax.broadcasted_iota(jnp.int32, (n, n), axis) for axis in (0, 1))


def newton_step(product, sym, low):
    i, j = square()
    inv = low[...]
    e = product(product(inv, sym[...], ((1,), (0,))), inv, ((1,), (1,)))
    e = e - jnp.where(i == j, 1.0, 0.0)
    phi = jnp.where(i > j, e, jnp.where(i == j, 0.5 * e, 0.0))
    low[...] = inv - product(phi, inv, ((1,), (0,)))
    return jnp.sum(e * e)


def fast_kernel(
    sizes, m_ref, g_ref, b_ref,
    buft_ref, p_ref, gram_ref, ortho_ref, right_ref, mom_ref, colsq_ref, err_ref,
    mv, gv, bv, buft, part, xbuf, zpart, zbuf, pbuf, gp, gbuf, gh, ybuf, gall, sym, low,
    obuf, rpart, cbuf, rhalf, wbuf, rall, sq1, sq2, mom,
    ins, store, xs, xr, zs, zr, zs2, zr2, xs2, xr2, cs, cr, ys, yr, ys2, yr2, cs2, cr2,
    cs3, cr3, ys3, yr3, ys4, yr4, cs4, cr4, s1, r1, s2, r2,
):
    nz, nx, ny, nc = sizes
    z, x, y, c = (lax.axis_index(a) for a in (Z, X, Y, C))
    loads = [pltpu.make_async_copy(a, b, ins.at[i]) for i, (a, b) in enumerate(((m_ref, mv), (g_ref, gv), (b_ref, bv)))]
    for cp in loads:
        cp.start()
    barrier = pltpu.get_barrier_semaphore()
    plane = far_pairs(ny, nx)
    line = far_pairs(nz, nc)
    for dz, dc in line:
        to = {Z: wrap(z + dz, nz), C: wrap(c + dc, nc)}
        pl.semaphore_signal(barrier, inc=1, device_id=to, device_id_type=MESH)
    for dy, dx in plane:
        to = {Y: wrap(y + dy, ny), X: wrap(x + dx, nx)}
        pl.semaphore_signal(barrier, inc=1, device_id=to, device_id_type=MESH)
    for cp in loads:
        cp.wait()

    buffer = (mv[...].astype(F32) + gv[...].astype(F32)).astype(BF)
    buft[...] = buffer
    part[...] = lax.dot_general(
        bv[...], buffer, (((0,), (0,)), ((), ())), preferred_element_type=F32
    ).astype(BF)
    outs = [pltpu.make_async_copy(buft, buft_ref, store.at[0])]
    outs[0].start()
    pl.semaphore_wait(barrier, len(plane) + len(line))

    q = part.shape[1] // nx
    th = RANK // nz
    order = far_first(nz) + [0]

    def tile(i, j):
        return (rows(i * th, th), rows(j * q, q))

    scatter = {}
    for e in order:
        to = wrap(z + e, nz)
        for d in far_first(nx):
            peer = wrap(x + d, nx)
            k = e * nx + d
            cp = remote(part.at[tile(to, peer)], xbuf.at[k], xs.at[k], xr.at[k], {X: peer})
            cp.start()
            scatter[k] = cp

    second = {}
    for e in order:
        to = wrap(z + e, nz)
        total = part[tile(to, x)].astype(F32)
        for d in far_first(nx):
            scatter[e * nx + d].wait_recv()
            total += xbuf[e * nx + d].astype(F32)
        if e:
            zpart[e] = total.astype(BF)
            second[e] = remote(zpart.at[e], zbuf.at[e], zs.at[e], zr.at[e], {Z: to})
            second[e].start()
        else:
            own = total
    for e in near_first(nz):
        second[e].wait_recv()
        own += zbuf[e].astype(F32)

    def forward(i):
        t = pbuf.at[tile(i, x)]
        for d in far_first(nx):
            remote(t, t, xs2.at[d], xr2.at[d], {X: wrap(x + d, nx)}).start()

    pbuf[tile(z, x)] = own.astype(BF)
    home = pbuf.at[tile(z, x)]
    gather = []
    for d in far_first(nz):
        cp = remote(home, home, zs2.at[d], zr2.at[d], {Z: wrap(z + d, nz)})
        cp.start()
        gather.append(cp)
    forward(z)
    for cp in list(scatter.values()) + list(second.values()):
        cp.wait_send()
    for d in near_first(nz):
        src = wrap(z - d + nz, nz)
        there = pbuf.at[tile(src, x)]
        remote(there, there, zs2.at[d], zr2.at[d], {Z: src}).wait_recv()
        forward(src)
    for cp in gather:
        cp.wait_send()

    def quarter(j):
        return (pl.ds(0, RANK), rows(j * q, q))

    for d in near_first(nx):
        src = wrap(x - d + nx, nx)
        there = pbuf.at[quarter(src)]
        remote(there, there, xs2.at[d], xr2.at[d], {X: src}).wait_recv()
    outs.append(pltpu.make_async_copy(pbuf, p_ref, store.at[1]))
    outs[1].start()
    b = RANK // 2
    gp[: 2 * b, :] = lanes(pbuf[...], pbuf[:b, :])
    gp[2 * b :, :] = lanes(pbuf[b:, :], pbuf[b:, :])

    h = 3 * b // 2
    peer = {C: 1 - c}
    cp = remote(gp.at[rows((1 - c) * h, h)], gbuf, cs, cr, peer)
    cp.start()
    for d in far_first(nx):
        mine = pbuf.at[quarter(x)]
        remote(mine, mine, xs2.at[d], xr2.at[d], {X: wrap(x + d, nx)}).wait_send()
    cp.wait()
    gh[...] = gp[rows(c * h, h), :] + gbuf[...]

    s = h // ny
    copies = []
    for d in far_first(ny):
        to = wrap(y + d, ny)
        cp = remote(gh.at[rows(to * s, s)], ybuf.at[d], ys.at[d], yr.at[d], {Y: to})
        cp.start()
        copies.append(cp)
    for cp in copies:
        cp.wait()
    own = gh[rows(y * s, s), :]
    for d in range(1, ny):
        own += ybuf[d]

    def slot(i):
        return rows(c * h + i * s, s)

    def across(i):
        t = gall.at[slot(i)]
        remote(t, t, cs2, cr2, peer).start()

    gall[slot(y), :] = own
    copies = []
    for d in far_first(ny):
        cp = remote(gall.at[slot(y)], gall.at[slot(y)], ys2.at[d], yr2.at[d], {Y: wrap(y + d, ny)})
        cp.start()
        copies.append(cp)
    across(y)
    for d in near_first(ny):
        src = wrap(y - d + ny, ny)
        remote(gall.at[slot(src)], gall.at[slot(src)], ys2.at[d], yr2.at[d], {Y: src}).wait_recv()
        across(src)
    for cp in copies:
        cp.wait_send()
    half = rows(c * h, h)
    remote(gall.at[half], gall.at[half], cs2, cr2, peer).wait_send()
    other = rows((1 - c) * h, h)
    remote(gall.at[other], gall.at[other], cs2, cr2, peer).wait_recv()
    outs.append(pltpu.make_async_copy(gall, gram_ref, store.at[2]))
    outs[2].start()

    corner = gall[b : 2 * b, :]
    sym[:b, :b] = gall[:b, :]
    sym[b:, :b] = corner
    sym[:b, b:] = corner.T
    sym[b:, b:] = gall[2 * b :, :]
    gram = sym[...]
    i, j = square()
    diag = jnp.where(i == j, gram, 0.0)
    scale = lax.rsqrt(jnp.sum(diag, axis=0, keepdims=True))
    down = lax.rsqrt(jnp.sum(diag, axis=1, keepdims=True))
    normed = gram * scale * down
    sym[...] = normed
    low[...] = jnp.where(i > j, -normed, jnp.where(i == j, 1.5 - 0.5 * normed, 0.0))
    newton_step(quick, sym, low)
    err_ref[...] = jnp.zeros((1, 128), F32) + newton_step(full, sym, low)
    inv = low[...] * scale
    hi = inv.astype(BF)
    lo = (inv - hi.astype(F32)).astype(BF)
    power = pbuf[...]
    ortho = jnp.dot(hi, power, preferred_element_type=F32)
    ortho += jnp.dot(lo, power, preferred_element_type=F32)
    ortho = ortho.astype(BF)
    obuf[...] = ortho
    outs.append(pltpu.make_async_copy(obuf, ortho_ref, store.at[3]))
    outs[3].start()
    cols = buft.shape[0]
    rpart[:cols, :] = lanes(buft[...], ortho).astype(BF)
    rpart[cols:, :] = jnp.zeros((PAD - cols, RANK), BF)

    h = PAD // 2
    peer = {C: 1 - c}
    cp = remote(rpart.at[rows((1 - c) * h, h)], cbuf, cs3, cr3, peer)
    cp.start()
    cp.wait()
    rhalf[...] = (rpart[rows(c * h, h), :].astype(F32) + cbuf[...].astype(F32)).astype(BF)

    s = h // ny
    copies = []
    for d in far_first(ny):
        to = wrap(y + d, ny)
        cp = remote(rhalf.at[rows(to * s, s)], wbuf.at[d], ys3.at[d], yr3.at[d], {Y: to})
        cp.start()
        copies.append(cp)
    for cp in copies:
        cp.wait()
    own = rhalf[rows(y * s, s), :].astype(F32)
    for d in range(1, ny):
        own += wbuf[d].astype(F32)

    sq1[0] = jnp.sum(own * own, axis=0, keepdims=True)
    first = []
    for dy, dx in plane:
        k = dy * nx + dx
        to = {Y: wrap(y + dy, ny), X: wrap(x + dx, nx)}
        cp = remote(sq1.at[0], sq1.at[k], s1.at[k], r1.at[k], to)
        cp.start()
        first.append(cp)

    def slot(i):
        return rows(c * h + i * s, s)

    for cp in first:
        cp.wait()
    sq2[0] = jnp.sum(sq1[...], axis=0)
    second = []
    for dz, dc in line:
        k = dz * nc + dc
        to = {Z: wrap(z + dz, nz), C: wrap(c + dc, nc)}
        cp = remote(sq2.at[0], sq2.at[k], s2.at[k], r2.at[k], to)
        cp.start()
        second.append(cp)

    rall[slot(y), :] = own.astype(BF)
    gather = []
    for d in far_first(ny):
        cp = remote(rall.at[slot(y)], rall.at[slot(y)], ys4.at[d], yr4.at[d], {Y: wrap(y + d, ny)})
        cp.start()
        gather.append(cp)

    for d, cp in zip(far_first(ny), gather):
        cp.wait_send()
        src = wrap(y - d + ny, ny)
        remote(rall.at[slot(src)], rall.at[slot(src)], ys4.at[d], yr4.at[d], {Y: src}).wait_recv()
    mine = rows(c * h, h)
    cp = remote(rall.at[mine], rall.at[mine], cs4, cr4, peer)
    cp.start()
    cp.wait_send()
    other = rows((1 - c) * h, h)
    remote(rall.at[other], rall.at[other], cs4, cr4, peer).wait_recv()
    outs.append(pltpu.make_async_copy(rall, right_ref, store.at[4]))
    outs[4].start()
    feedback = jnp.dot(rall[:cols, :], ortho, preferred_element_type=F32)
    mom[...] = (buft[...].astype(F32) - 0.5 * feedback).astype(BF)
    outs.append(pltpu.make_async_copy(mom, mom_ref, store.at[5]))
    outs[5].start()
    for cp in second:
        cp.wait()
    colsq_ref[...] = jnp.sum(sq2[...], axis=0)
    for cp in outs:
        cp.wait()


def direct_kernel(g_ref, inv_ref, work):
    n = RANK
    i, j = square()
    gram = g_ref[...]
    diag = jnp.where(i == j, gram, 0.0)
    across = lax.rsqrt(jnp.sum(diag, axis=0, keepdims=True))
    down = lax.rsqrt(jnp.sum(diag, axis=1, keepdims=True))
    work[...] = gram * across * down
    inv_ref[...] = jnp.where(i == j, 1.0, 0.0)
    lane = lax.broadcasted_iota(jnp.int32, (1, n), 1)
    line = lax.broadcasted_iota(jnp.int32, (n, 1), 0)

    def column(k, _):
        pivots = work[pl.ds(k, 1), :]
        pivot = jnp.sum(jnp.where(lane == k, pivots, 0.0), axis=1, keepdims=True)
        inverse = inv_ref[pl.ds(k, 1), :]
        here = work[...]
        col = jnp.sum(jnp.where(j == k, here, 0.0), axis=1, keepdims=True)
        times = jnp.where(line > k, col / pivot, 0.0)
        work[...] = here - times * pivots
        inv_ref[...] = inv_ref[...] - times * inverse
        return 0

    lax.fori_loop(0, n, column, 0)
    pivot = jnp.sum(jnp.where(i == j, work[...], 0.0), axis=1, keepdims=True)
    inv_ref[...] = inv_ref[...] * lax.rsqrt(pivot) * across


def update_kernel(
    ortho_ref, right_ref, colsq_ref, mom_ref, w_ref, weight_ref, momentum_ref, basis_ref, wv, bv, outs
):
    first = pltpu.make_async_copy(mom_ref, momentum_ref, outs.at[0])
    first.start()
    cols = wv.shape[0]
    length = jnp.sqrt(colsq_ref[...] + 1e-06)
    basis = (right_ref[:cols, :].astype(F32) / length).astype(BF)
    bv[...] = basis
    second = pltpu.make_async_copy(bv, basis_ref, outs.at[1])
    second.start()
    coeff = 0.3 * (D * FF / RANK) ** 0.5 / 50.0
    update = jnp.dot(basis, ortho_ref[...], preferred_element_type=F32)
    wv[...] = (w_ref[...].astype(F32) - coeff * update).astype(BF)
    third = pltpu.make_async_copy(wv, weight_ref, outs.at[2])
    third.start()
    for cp in (first, second, third):
        cp.wait()


def vmem(n):
    return [pl.BlockSpec(memory_space=pltpu.VMEM)] * n


def anywhere(n):
    return [pl.BlockSpec(memory_space=pl.ANY)] * n


def bf(*shape):
    return jax.ShapeDtypeStruct(shape, BF)


def f32(*shape):
    return jax.ShapeDtypeStruct(shape, F32)


def finish(ortho, right, colsq, mom, weight):
    cols, nloc = mom.shape
    return pl.pallas_call(
        update_kernel,
        out_shape=(bf(cols, nloc), bf(cols, nloc), bf(cols, RANK)),
        in_specs=vmem(5),
        out_specs=tuple(anywhere(3)),
        scratch_shapes=[pltpu.VMEM((cols, nloc), BF), pltpu.VMEM((cols, RANK), BF), pltpu.SemaphoreType.DMA((3,))],
    )(ortho, right, colsq, mom, weight)


def general(sizes, buft, power, gram, weight):
    b = RANK // 2
    corner = gram[b : 2 * b]
    upper = jnp.concatenate([gram[:b], corner.T], axis=1)
    lower = jnp.concatenate([corner, gram[2 * b :]], axis=1)
    inv = pl.pallas_call(
        direct_kernel,
        out_shape=f32(RANK, RANK),
        in_specs=vmem(1),
        out_specs=vmem(1)[0],
        scratch_shapes=[pltpu.VMEM((RANK, RANK), F32)],
    )(jnp.concatenate([upper, lower]))
    hi = inv.astype(BF)
    lo = (inv - hi.astype(F32)).astype(BF)
    ortho = jnp.dot(hi, power, preferred_element_type=F32)
    ortho = (ortho + jnp.dot(lo, power, preferred_element_type=F32)).astype(BF)
    right = jnp.einsum("cr,kr->ck", buft, ortho, preferred_element_type=F32)
    pieces = right.reshape(sizes[2] * sizes[3], -1, RANK)
    share = jnp.sum(lax.all_to_all(pieces, ROW, 0, 0, tiled=True), axis=0)
    whole = lax.all_gather(share.astype(BF), ROW, tiled=True)
    colsq = jnp.sum(share * share, axis=0, keepdims=True)
    colsq = jnp.sum(lax.all_gather(colsq, ROW, tiled=True), axis=0, keepdims=True)
    colsq = jnp.sum(lax.all_gather(colsq, FSDP, tiled=True), axis=0, keepdims=True)
    feedback = jnp.dot(whole, ortho, preferred_element_type=F32)
    mom = (buft.astype(F32) - 0.5 * feedback).astype(BF)
    whole = jnp.pad(whole, ((0, PAD - whole.shape[0]), (0, 0)))
    return finish(ortho, whole, colsq, mom, weight)


def per_device(sizes, weight, momentum, gradient, basis):
    nz, nx, ny, nc = sizes
    nloc, cols = momentum.shape
    q = nloc // nx
    th = RANK // nz
    b = RANK // 2
    h = 3 * b // 2
    s = PAD // 2 // ny
    dma = pltpu.SemaphoreType.DMA
    scratch = [
        bf(cols, nloc), bf(cols, nloc), bf(cols, RANK), bf(cols, nloc), bf(RANK, nloc),
        bf(nx * nz, th, q), bf(nz, th, q), bf(nz, th, q), bf(RANK, nloc),
        f32(3 * b, b), f32(h, b), f32(h, b), f32(ny, h // ny, b), f32(3 * b, b), f32(RANK, RANK), f32(RANK, RANK),
        bf(RANK, nloc), bf(PAD, RANK), bf(PAD // 2, RANK), bf(PAD // 2, RANK), bf(ny, s, RANK), bf(PAD, RANK),
        f32(ny * nx, 1, RANK), f32(nz * nc, 1, RANK), bf(cols, nloc),
    ]
    buft, power, gram, ortho, right, mom, colsq, err = pl.pallas_call(
        functools.partial(fast_kernel, sizes),
        out_shape=(
            bf(cols, nloc), bf(RANK, nloc), f32(3 * b, b), bf(RANK, nloc), bf(PAD, RANK), bf(cols, nloc),
            f32(1, RANK), f32(1, 128),
        ),
        in_specs=anywhere(3),
        out_specs=tuple(anywhere(6) + vmem(2)),
        scratch_shapes=[pltpu.VMEM(v.shape, v.dtype) for v in scratch] + [
            dma((3,)), dma((6,)), dma((nx * nz,)), dma((nx * nz,)),
            dma((nz,)), dma((nz,)), dma((nz,)), dma((nz,)), dma((nx,)), dma((nx,)),
            dma, dma, dma((ny,)), dma((ny,)), dma((ny,)), dma((ny,)), dma, dma,
            dma, dma, dma((ny,)), dma((ny,)), dma((ny,)), dma((ny,)), dma, dma,
            dma((ny * nx,)), dma((ny * nx,)), dma((nz * nc,)), dma((nz * nc,)),
        ],
        compiler_params=pltpu.CompilerParams(collective_id=0, has_side_effects=True),
    )(momentum.T, gradient.T, basis)

    weight_new, momentum_new, basis_new = lax.cond(
        err[0, 0] <= SMALL,
        lambda: finish(ortho, right, colsq, mom, weight.T),
        lambda: general(sizes, buft, power, gram, weight.T),
    )
    return weight_new.T, momentum_new.T, basis_new


def build(devices, sizes):
    finer = Mesh(devices.reshape(sizes), (Z, X, Y, C))
    return jax.shard_map(
        functools.partial(per_device, sizes),
        mesh=finer,
        in_specs=(P(ROW, FSDP), P(ROW, FSDP), P(ROW, FSDP), P(FSDP, None)),
        out_specs=(P(ROW, FSDP), P(ROW, FSDP), P(FSDP, None)),
        check_vma=False,
    )


def solution(mesh):
    return build(mesh.devices, SIZES)
```
